512 devices in a mesh: expert: 64 (over z_lo, y, x), shard: 8 (over z_hi, core).
Axes of the slice: x: 4, y: 8, z: 8 (z_hi: 4, z_lo: 2; z = z_hi * 2 + z_lo), core: 2. Of those that a mesh axis runs over, the one named last changes fastest.
Arguments:
- w_gate: float32 [64, 2048, 1024], P('expert', 'shard'), may hold values from -0.125 to 0.125
- avg_gate: float32 [64, 2048, 1024], P('expert', 'shard'), may hold values from -0.125 to 0.125
- w_up: float32 [64, 2048, 1024], P('expert', 'shard'), may hold values from -0.125 to 0.125
- avg_up: float32 [64, 2048, 1024], P('expert', 'shard'), may hold values from -0.125 to 0.125
- mix_share: float32 [64], P('expert'), may hold values from 0.2 to 0.8
- router_weight: float32 [2048, 64], P('shard', 'expert'), may hold values from -0.125 to 0.125
- router_gain: float32 [2048], P('shard'), may hold values from 0.25 to 1.75
Outputs:
- serve_gate: bfloat16 [64, 1024, 2048], P('expert')
- serve_up: bfloat16 [64, 1024, 2048], P('expert')
- serve_router: bfloat16 [2048, 64], replicated
The draws below stay inside these ranges and needn't reach their ends.
All inputs are finite; a program needn't handle non-finite values.
Results may differ from the reference program's by a relative error of at most 0.001.
Values may be sent and summed in bfloat16 or wider, within the bound.
No kernel may reach another device: no remote copies, remote signals or barrier semaphores. Data moves between devices by JAX's collectives and lax.ppermute only.
A program may use at most 64 MiB of HBM per device.

```python
import jax
import jax.numpy as jnp

EXPERTS = 64
D_MODEL = 2048
D_EXPERT = 1024


def levels(own_key, dims, pieces, low, top_value):
    level, own = 1.0, jax.random.fold_in(own_key, 6)
    for position, parts in pieces:
        draws = jnp.exp(jax.random.uniform(jax.random.fold_in(own, position), (parts,), jnp.float32, low / len(pieces), top_value / len(pieces)))
        level = level * jnp.repeat(draws, dims[position] // parts).reshape([-1 if axis == position else 1 for axis in range(len(dims))])
    return level


def gaussian(key, extent, scale, most, cuts=(), kind=jnp.bfloat16):
    level = levels(key, extent, cuts, -0.22, 0.18) if cuts else 1.0
    values = jax.random.normal(key, extent, jnp.float32) * scale * level
    return jnp.minimum(jnp.maximum(values, -most), most).astype(kind)


def setup_inputs(seed: int = 0) -> dict:
    streams_of = jax.random.split(jax.random.key(seed), 8)
    return {
        "w_gate": gaussian(streams_of[0], (EXPERTS, D_MODEL, D_EXPERT), D_MODEL ** -0.5, 0.125, ((0, 64), (1, 8)), jnp.float32),
        "avg_gate": gaussian(streams_of[1], (EXPERTS, D_MODEL, D_EXPERT), D_MODEL ** -0.5, 0.125, ((0, 64), (1, 8)), jnp.float32),
        "w_up": gaussian(streams_of[2], (EXPERTS, D_MODEL, D_EXPERT), D_MODEL ** -0.5, 0.125, ((0, 64), (1, 8)), jnp.float32),
        "avg_up": gaussian(streams_of[3], (EXPERTS, D_MODEL, D_EXPERT), D_MODEL ** -0.5, 0.125, ((0, 64), (1, 8)), jnp.float32),
        "mix_share": jnp.clip(0.2 + 0.6 * jax.random.uniform(streams_of[4], (EXPERTS,), jnp.float32) ** levels(streams_of[4], (EXPERTS,), ((0, 64),), -0.2, 0.2), 0.2, 0.8),
        "router_weight": gaussian(streams_of[5], (D_MODEL, EXPERTS), D_MODEL ** -0.5, 0.125, ((0, 8), (1, 64)), jnp.float32),
        "router_gain": jnp.clip(1.0 + 0.15 * jax.random.normal(streams_of[6], (D_MODEL,), jnp.float32), 0.25, 1.75),
    }


def reference(w_gate, avg_gate, w_up, avg_up, mix_share, router_weight, router_gain):
    fresh_gate = mix_share[:, None, None] * w_gate + (1.0 - mix_share[:, None, None]) * avg_gate
    fresh_up = mix_share[:, None, None] * w_up + (1.0 - mix_share[:, None, None]) * avg_up
    serve_gate = fresh_gate.astype(jnp.bfloat16)
    serve_gate = jnp.transpose(serve_gate, (0, 2, 1))
    serve_up = fresh_up.astype(jnp.bfloat16)
    serve_up = jnp.transpose(serve_up, (0, 2, 1))
    serve_router = (router_weight * router_gain[:, None]).astype(jnp.bfloat16)
    return serve_gate, serve_up, serve_router
```

```python
import functools

import jax
import jax.numpy as jnp
from jax import lax
from jax.experimental import pallas as pl
from jax.experimental.pallas import tpu as pltpu
from jax.sharding import Mesh
from jax.sharding import PartitionSpec as P


BF16 = jnp.bfloat16
PIECES = 4
EXPERT = ("zlo", "y", "x")
SHARD = ("zhi", "core")
ANY = pl.BlockSpec(memory_space=pl.ANY)
HBM = pl.BlockSpec(memory_space=pltpu.HBM)
VMEM = pl.BlockSpec(memory_space=pltpu.VMEM)
SMEM = pl.BlockSpec(memory_space=pltpu.SMEM)
GATE, UP = 0, 1


def mix_kernel(share_ref, w_ref, avg_ref, *refs):
    before, outs, (buf, sems) = refs[:-4], refs[-4:-2], refs[-2:]
    rows = w_ref.shape[1]
    width = rows // PIECES

    def copies(piece):
        cols = pl.ds(piece * width, width)
        return [
            pltpu.make_async_copy(src.at[:, cols], buf.at[i, piece], sems.at[i, piece])
            for i, src in enumerate((w_ref, avg_ref))
        ]

    for piece in range(PIECES):
        for c in copies(piece):
            c.start()
    share = share_ref[0]
    rest = 1.0 - share
    for piece in range(PIECES):
        for c in copies(piece):
            c.wait()
        fresh = share * buf[0, piece] + rest * buf[1, piece]
        turned = fresh.T.astype(BF16)
        outs[0][pl.ds(piece * width, width), :] = turned
        if before:
            outs[1][pl.ds(piece * width, width), :] = before[0][pl.ds(piece * width, width), :]
            outs[1][pl.ds(rows + piece * width, width), :] = turned


def first_kernel(share_ref, w_ref, avg_ref, out_ref, buf, sems):
    mix_kernel(share_ref, w_ref, avg_ref, out_ref, None, buf, sems)


def mixed(share, w, avg, before=None):
    rows, cols = w.shape
    w, avg = (pltpu.with_memory_space_constraint(x, pltpu.HBM) for x in (w, avg))
    extra = () if before is None else (pltpu.with_memory_space_constraint(before, pltpu.VMEM),)
    return pl.pallas_call(
        mix_kernel if extra else first_kernel,
        out_shape=(pltpu.VMEM((cols, rows), BF16),) + ((pltpu.VMEM((2 * cols, rows), BF16),) if extra else ()),
        in_specs=[SMEM, HBM, HBM] + [VMEM] * len(extra),
        out_specs=(VMEM,) * (1 + len(extra)),
        scratch_shapes=[
            pltpu.VMEM((2, PIECES, rows, cols // PIECES), jnp.float32),
            pltpu.SemaphoreType.DMA((2, PIECES)),
        ],
        compiler_params=pltpu.CompilerParams(vmem_limit_bytes=12 << 20),
        cost_estimate=pl.CostEstimate(flops=4 * rows * cols, bytes_accessed=10 * rows * cols, transcendentals=0),
        name="mix",
    )(share, w, avg, *extra)


def place_kernel(counts, by, join, *refs):
    outs, sems = refs[-3 - join : -1 - join], refs[-1]
    joined = refs[-2] if join else None
    width = refs[0].shape[1]
    chips = lax.axis_size("zhi")
    chip, core = lax.axis_index("zhi"), lax.axis_index("core")
    sign = 1 - 2 * lax.axis_index("zlo")
    copies, pieces, at = [], [], 0
    entries = iter(by)
    for ref, count in zip(refs, counts):
        row = 0
        for _ in range(count):
            which, start, size, step, other = next(entries)
            owner = lax.rem(chip + chips - step * sign, chips) * 2 + (1 - core if other else core)
            cols = pl.ds(pl.multiple_of(owner * width, width), width)
            piece = ref.at[pl.ds(row, size), :]
            row += size
            pieces.append((piece, size))
            copies.append(pltpu.make_async_copy(piece, outs[which].at[pl.ds(start, size), cols], sems.at[len(copies)]))
    for c in copies:
        c.start()
    if join:
        for piece, size in pieces:
            joined[pl.ds(at, size), :] = piece[...]
            at += size
    for c in copies:
        c.wait()


def placed(outs, arrays, columns, rows, join=False):
    n = len(arrays)
    by = tuple(p for _, pieces in arrays for p in pieces)
    counts = tuple(len(pieces) for _, pieces in arrays)
    arrays = [pltpu.with_memory_space_constraint(a, pltpu.VMEM) for a, _ in arrays]
    width = arrays[0].shape[1]
    total = sum(p[2] for p in by)
    out = jax.ShapeDtypeStruct((rows, columns), BF16)
    extra = () if outs is None else tuple(outs)
    res = pl.pallas_call(
        functools.partial(place_kernel, counts, by, int(join)),
        out_shape=(out, out) + ((pltpu.VMEM((total, width), BF16),) if join else ()),
        in_specs=[VMEM] * n + [ANY] * len(extra),
        out_specs=(ANY, ANY) + ((VMEM,) if join else ()),
        input_output_aliases={n + i: i for i in range(len(extra))},
        scratch_shapes=[pltpu.SemaphoreType.DMA((len(by),))],
        compiler_params=pltpu.CompilerParams(vmem_limit_bytes=12 << 20),
        cost_estimate=pl.CostEstimate(flops=2 * total * width, bytes_accessed=4 * total * width, transcendentals=0),
        name="place",
    )(*arrays, *extra)
    return res[:2], (res[2] if join else None)


def order_kernel(nx, ny, nz, in_ref, out_ref, wide, turned):
    lanes = in_ref.shape[1]
    wide[...] = in_ref[...].astype(jnp.float32)
    shards = in_ref.shape[0] // (nx * ny * nz * 2)
    for x in range(nx):
        for z in range(nz):
            for s in range(shards):
                for h in range(2):
                    rows = wide[pl.ds(((x * nz + z) * shards + s) * ny * 2 + h, ny, stride=2), :]
                    turned[s * 2 + h, pl.ds(z * ny * nx + x, ny, stride=nx), :] = rows
    for j in range(2 * shards):
        out_ref[:, pl.ds(j * lanes, lanes)] = turned[j].astype(BF16)


def ordered(part, nx, ny, nz):
    rows, lanes = part.shape
    experts = nx * ny * nz
    return pl.pallas_call(
        functools.partial(order_kernel, nx, ny, nz),
        out_shape=jax.ShapeDtypeStruct((experts, rows * lanes // experts), BF16),
        in_specs=[VMEM],
        out_specs=VMEM,
        scratch_shapes=[
            pltpu.VMEM((rows, lanes), jnp.float32),
            pltpu.VMEM((rows // experts, experts, lanes), jnp.float32),
        ],
        compiler_params=pltpu.CompilerParams(vmem_limit_bytes=4 << 20),
        cost_estimate=pl.CostEstimate(flops=rows * lanes, bytes_accessed=4 * rows * lanes, transcendentals=0),
        name="order",
    )(part)


def spread(x, axes):
    n = lax.axis_size(axes)
    return lax.all_to_all(jnp.broadcast_to(x[None], (n, *x.shape)), axes, 0, 0, tiled=True)


def local(w_gate, avg_gate, w_up, avg_up, mix_share, router_weight, router_gain):
    chips = lax.axis_size("zhi")
    columns = w_gate.shape[1] * chips * lax.axis_size("core")
    rows = w_gate.shape[2]

    def moved(x, by):
        pairs = [
            (lo * chips + hi, lo * chips + (hi + (by if lo == 0 else -by)) % chips) for lo in range(2) for hi in range(chips)
        ]
        return lax.ppermute(x, ("zlo", "zhi"), pairs)

    def partner(x):
        return lax.ppermute(x, "core", [(0, 1), (1, 0)])

    def place(outs, *arrays, join=False):
        return placed(outs, arrays, columns, rows, join)

    def pieces(step, other, *which):
        return tuple((w, 0, rows, step, other) for w in which)

    (gate,) = mixed(mix_share, w_gate[0], avg_gate[0])
    up, own = mixed(mix_share, w_up[0], avg_up[0], gate)
    a1 = moved(gate, 1)
    a2 = moved(up, 1)
    c1 = moved(a1, 1)
    c2 = moved(a2, 1)
    b1 = moved(gate, -1)
    b2 = moved(up, -1)

    nx, ny, nz = (lax.axis_size(a) for a in ("x", "y", "zlo"))
    part = (router_weight * router_gain[:, None]).astype(BF16).reshape(2, -1)
    lanes = part.shape[1]
    part = spread(part, ("y",)).reshape(-1, lanes)
    part = spread(part, ("zlo", "zhi", "core")).reshape(-1, lanes)
    part = spread(part, ("x",)).reshape(-1, lanes)
    serve_router = ordered(part, nx, ny, nz).T

    outs, _ = place(None, (own, pieces(0, 0, GATE, UP)))
    outs, _ = place(outs, (partner(own), pieces(0, 1, GATE, UP)))
    outs, both = place(outs, (a1, pieces(1, 0, GATE)), (a2, pieces(1, 0, UP)), join=True)
    outs, _ = place(outs, (partner(both), pieces(1, 1, GATE, UP)))
    c1_other = partner(c1)
    b1_other = partner(b1)
    b2_other = partner(b2)
    c2_other = partner(c2)
    outs, _ = place(outs, (c1, pieces(2, 0, GATE)), (c1_other, pieces(2, 1, GATE)), (b1, pieces(-1, 0, GATE)))
    outs, _ = place(outs, (b1_other, pieces(-1, 1, GATE)), (b2, pieces(-1, 0, UP)), (c2, pieces(2, 0, UP)))
    outs, _ = place(outs, (b2_other, pieces(-1, 1, UP)), (c2_other, pieces(2, 1, UP)))
    return outs[0][None], outs[1][None], serve_router


def solution(mesh):
    devices = mesh.devices.reshape(2, 8, 4, 4, 2)
    split = Mesh(devices, EXPERT + SHARD)
    return jax.shard_map(
        local,
        mesh=split,
        in_specs=(
            P(EXPERT, SHARD, None),
            P(EXPERT, SHARD, None),
            P(EXPERT, SHARD, None),
            P(EXPERT, SHARD, None),
            P(EXPERT),
            P(SHARD, EXPERT),
            P(SHARD),
        ),
        out_specs=(P(EXPERT, None, None), P(EXPERT, None, None), P()),
        check_vma=False,
    )
```

```python
import functools

import jax
import jax.numpy as jnp
from jax import lax
from jax.experimental import pallas as pl
from jax.experimental.pallas import tpu as pltpu
from jax.sharding import Mesh
from jax.sharding import PartitionSpec as P


BF16 = jnp.bfloat16
PIECES = 4
EXPERT = ("zlo", "y", "x")
SHARD = ("zhi", "core")
ANY = pl.BlockSpec(memory_space=pl.ANY)
HBM = pl.BlockSpec(memory_space=pltpu.HBM)
VMEM = pl.BlockSpec(memory_space=pltpu.VMEM)
SMEM = pl.BlockSpec(memory_space=pltpu.SMEM)
GATE, UP = 0, 1
AHEAD = -1


def mix_kernel(share_ref, w_ref, avg_ref, *refs):
    before, outs, (buf, sems) = refs[:-4], refs[-4:-2], refs[-2:]
    rows = w_ref.shape[1]
    width = rows // PIECES

    def copies(piece):
        cols = pl.ds(piece * width, width)
        return [
            pltpu.make_async_copy(src.at[:, cols], buf.at[i, piece], sems.at[i, piece])
            for i, src in enumerate((w_ref, avg_ref))
        ]

    for piece in range(PIECES):
        for c in copies(piece):
            c.start()
    share = share_ref[0]
    rest = 1.0 - share
    for piece in range(PIECES):
        for c in copies(piece):
            c.wait()
        fresh = share * buf[0, piece] + rest * buf[1, piece]
        turned = fresh.T.astype(BF16)
        outs[0][pl.ds(piece * width, width), :] = turned
        if before:
            outs[1][pl.ds(piece * width, width), :] = before[0][pl.ds(piece * width, width), :]
            outs[1][pl.ds(rows + piece * width, width), :] = turned


def first_kernel(share_ref, w_ref, avg_ref, out_ref, buf, sems):
    mix_kernel(share_ref, w_ref, avg_ref, out_ref, None, buf, sems)


def mixed(share, w, avg, before=None):
    rows, cols = w.shape
    w, avg = (pltpu.with_memory_space_constraint(x, pltpu.HBM) for x in (w, avg))
    extra = () if before is None else (pltpu.with_memory_space_constraint(before, pltpu.VMEM),)
    return pl.pallas_call(
        mix_kernel if extra else first_kernel,
        out_shape=(pltpu.VMEM((cols, rows), BF16),) + ((pltpu.VMEM((2 * cols, rows), BF16),) if extra else ()),
        in_specs=[SMEM, HBM, HBM] + [VMEM] * len(extra),
        out_specs=(VMEM,) * (1 + len(extra)),
        scratch_shapes=[
            pltpu.VMEM((2, PIECES, rows, cols // PIECES), jnp.float32),
            pltpu.SemaphoreType.DMA((2, PIECES)),
        ],
        compiler_params=pltpu.CompilerParams(vmem_limit_bytes=12 << 20),
        cost_estimate=pl.CostEstimate(flops=4 * rows * cols, bytes_accessed=10 * rows * cols, transcendentals=0),
        name="mix",
    )(share, w, avg, *extra)


def place_kernel(counts, by, join, *refs):
    extra = 1 if join else 0
    outs, sems = refs[-3 - extra : -1 - extra], refs[-1]
    joined = refs[-2] if join else None
    width = refs[0].shape[1]
    chips = lax.axis_size("zhi")
    chip, core = lax.axis_index("zhi"), lax.axis_index("core")
    sign = AHEAD * (1 - 2 * lax.axis_index("zlo"))
    copies, pieces, at = [], [], 0
    entries = iter(by)
    for ref, count in zip(refs, counts):
        row = 0
        for _ in range(count):
            which, start, size, step, other = next(entries)
            owner = lax.rem(chip + chips - step * sign, chips) * 2 + (1 - core if other else core)
            cols = pl.ds(pl.multiple_of(owner * width, width), width)
            piece = ref.at[pl.ds(row, size), :]
            row += size
            pieces.append((piece, size))
            copies.append(pltpu.make_async_copy(piece, outs[which].at[pl.ds(start, size), cols], sems.at[len(copies)]))
    for c in copies:
        c.start()
    if join:
        for piece, size in pieces[:join]:
            joined[pl.ds(at, size), :] = piece[...]
            at += size
    for c in copies:
        c.wait()


def placed(outs, arrays, columns, rows, join=0):
    n = len(arrays)
    by = tuple(p for _, pieces in arrays for p in pieces)
    counts = tuple(len(pieces) for _, pieces in arrays)
    arrays = [pltpu.with_memory_space_constraint(a, pltpu.VMEM) for a, _ in arrays]
    width = arrays[0].shape[1]
    total = sum(p[2] for p in by)
    joined = sum(p[2] for p in by[:join])
    out = jax.ShapeDtypeStruct((rows, columns), BF16)
    extra = () if outs is None else tuple(outs)
    res = pl.pallas_call(
        functools.partial(place_kernel, counts, by, join),
        out_shape=(out, out) + ((pltpu.VMEM((joined, width), BF16),) if join else ()),
        in_specs=[VMEM] * n + [ANY] * len(extra),
        out_specs=(ANY, ANY) + ((VMEM,) if join else ()),
        input_output_aliases={n + i: i for i in range(len(extra))},
        scratch_shapes=[pltpu.SemaphoreType.DMA((len(by),))],
        compiler_params=pltpu.CompilerParams(vmem_limit_bytes=12 << 20),
        cost_estimate=pl.CostEstimate(flops=2 * total * width, bytes_accessed=4 * total * width, transcendentals=0),
        name="place",
    )(*arrays, *extra)
    return res[:2], (res[2] if join else None)


def order_kernel(nxy, nz, in_ref, out_ref, wide):
    lanes = in_ref.shape[1]
    wide[...] = in_ref[...].astype(jnp.float32)
    column = in_ref.shape[0] // nxy
    for z in range(nz):
        for j in range(column // nz):
            rows = wide[pl.ds(z * (column // nz) + j, nxy, stride=column), :]
            out_ref[pl.ds(z * nxy, nxy), pl.ds(j * lanes, lanes)] = rows.astype(BF16)


def ordered(part, nxy, nz):
    rows, lanes = part.shape
    experts = nxy * nz
    return pl.pallas_call(
        functools.partial(order_kernel, nxy, nz),
        out_shape=jax.ShapeDtypeStruct((experts, rows * lanes // experts), BF16),
        in_specs=[VMEM],
        out_specs=VMEM,
        scratch_shapes=[
            pltpu.VMEM((rows, lanes), jnp.float32),
        ],
        compiler_params=pltpu.CompilerParams(vmem_limit_bytes=4 << 20),
        cost_estimate=pl.CostEstimate(flops=rows * lanes, bytes_accessed=4 * rows * lanes, transcendentals=0),
        name="order",
    )(part)


def spread(x, axes):
    n = lax.axis_size(axes)
    return lax.all_to_all(jnp.broadcast_to(x[None], (n, *x.shape)), axes, 0, 0, tiled=True)


def local(w_gate, avg_gate, w_up, avg_up, mix_share, router_weight, router_gain):
    chips = lax.axis_size("zhi")
    columns = w_gate.shape[1] * chips * lax.axis_size("core")
    rows = w_gate.shape[2]

    def moved(x, by):
        pairs = [
            (lo * chips + hi, lo * chips + (hi + (by if lo == 0 else -by)) % chips) for lo in range(2) for hi in range(chips)
        ]
        return lax.ppermute(x, ("zlo", "zhi"), pairs)

    def partner(x):
        return lax.ppermute(x, "core", [(0, 1), (1, 0)])

    def place(outs, *arrays, join=0):
        return placed(outs, arrays, columns, rows, join)

    def pieces(step, other, *which):
        return tuple((w, 0, rows, step, other) for w in which)

    (gate,) = mixed(mix_share, w_gate[0], avg_gate[0])
    up, own = mixed(mix_share, w_up[0], avg_up[0], gate)
    a1 = moved(gate, AHEAD)
    a2 = moved(up, AHEAD)
    c1 = moved(a1, AHEAD)
    c2 = moved(a2, AHEAD)
    f1 = moved(c1, AHEAD)
    f2 = moved(c2, AHEAD)

    nx, ny, nz = (lax.axis_size(a) for a in ("x", "y", "zlo"))
    part = (router_weight * router_gain[:, None]).astype(BF16).reshape(2, -1)
    lanes = part.shape[1]
    part = spread(part, ("zlo", "zhi", "core")).reshape(-1, lanes)
    part = spread(part, ("y", "x")).reshape(-1, lanes)
    serve_router = ordered(part, nx * ny, nz).T

    outs, _ = place(None, (own, pieces(0, 0, GATE, UP)))
    outs, both = place(
        outs, (a1, pieces(1, 0, GATE)), (a2, pieces(1, 0, UP)), (partner(own), pieces(0, 1, GATE, UP)), join=2
    )
    outs, _ = place(outs, (partner(both), pieces(1, 1, GATE, UP)))
    outs, both = place(outs, (c1, pieces(2, 0, GATE)), (c2, pieces(2, 0, UP)), join=2)
    both_other, f1_other, f2_other = partner(both), partner(f1), partner(f2)
    outs, _ = place(outs, (both_other, pieces(2, 1, GATE, UP)), (f1, pieces(3, 0, GATE)))
    outs, _ = place(outs, (f1_other, pieces(3, 1, GATE)), (f2, pieces(3, 0, UP)))
    outs, _ = place(outs, (f2_other, pieces(3, 1, UP)))
    return outs[0][None], outs[1][None], serve_router


def solution(mesh):
    devices = mesh.devices.reshape(2, 8, 4, 4, 2)
    split = Mesh(devices, EXPERT + SHARD)
    return jax.shard_map(
        local,
        mesh=split,
        in_specs=(
            P(EXPERT, SHARD, None),
            P(EXPERT, SHARD, None),
            P(EXPERT, SHARD, None),
            P(EXPERT, SHARD, None),
            P(EXPERT),
            P(SHARD, EXPERT),
            P(SHARD),
        ),
        out_specs=(P(EXPERT, None, None), P(EXPERT, None, None), P()),
        check_vma=False,
    )
```

```python
import functools

import jax
import jax.numpy as jnp
from jax import lax
from jax.experimental import pallas as pl
from jax.experimental.pallas import tpu as pltpu
from jax.sharding import Mesh
from jax.sharding import PartitionSpec as P


BF16 = jnp.bfloat16
WIDTH = 256
HEAD = 256
FIRST = 512
EXPERT = ("zlo", "y", "x")
SHARD = ("zhi", "core")
ANY = pl.BlockSpec(memory_space=pl.ANY)
HBM = pl.BlockSpec(memory_space=pltpu.HBM)
VMEM = pl.BlockSpec(memory_space=pltpu.VMEM)
SMEM = pl.BlockSpec(memory_space=pltpu.SMEM)
GATE, UP = 0, 1
AHEAD = -1


def mix_kernel(plan, share_ref, *refs):
    n = len(plan)
    sources, before, outs, (buf, sems) = refs[: 2 * n], refs[2 * n : -4], refs[-4:-2], refs[-2:]
    width = buf.shape[-1]
    chunks, row = [], 0
    for i, (first, size) in enumerate(plan):
        for col in range(first, first + size, width):
            chunks.append((sources[2 * i], sources[2 * i + 1], col, min(width, first + size - col), row))
            row += chunks[-1][3]

    def copies(k):
        w, avg, col, size, _ = chunks[k]
        return [
            pltpu.make_async_copy(src.at[:, pl.ds(col, size)], buf.at[i, k, :, pl.ds(0, size)], sems.at[i, k])
            for i, src in enumerate((w, avg))
        ]

    for k in range(len(chunks)):
        for c in copies(k):
            c.start()
    share = share_ref[0]
    rest = 1.0 - share
    for k, (_, _, _, size, at) in enumerate(chunks):
        for c in copies(k):
            c.wait()
        fresh = share * buf[0, k, :, :size] + rest * buf[1, k, :, :size]
        turned = fresh.astype(BF16).T
        outs[0][pl.ds(at, size), :] = turned
        if before:
            outs[1][pl.ds(before[0].shape[0] + at, size), :] = turned
    if before:
        outs[1][pl.ds(0, before[0].shape[0]), :] = before[0][...]


def first_kernel(plan, *refs):
    mix_kernel(plan, *refs[:-2], None, *refs[-2:])


def mixed(share, sources, before=None):
    rows = sources[0][0].shape[0]
    plan = tuple((first, size) for _, _, first, size in sources)
    total = sum(size for _, size in plan)
    arrays = [pltpu.with_memory_space_constraint(x, pltpu.HBM) for w, avg, _, _ in sources for x in (w, avg)]
    extra = () if before is None else (pltpu.with_memory_space_constraint(before, pltpu.VMEM),)
    chunks = sum(-(-size // WIDTH) for _, size in plan)
    return pl.pallas_call(
        functools.partial(mix_kernel if extra else first_kernel, plan),
        out_shape=(pltpu.VMEM((total, rows), BF16),)
        + ((pltpu.VMEM((before.shape[0] + total, rows), BF16),) if extra else ()),
        in_specs=[SMEM] + [HBM] * len(arrays) + [VMEM] * len(extra),
        out_specs=(VMEM,) * (1 + len(extra)),
        scratch_shapes=[
            pltpu.VMEM((2, chunks, rows, WIDTH), jnp.float32),
            pltpu.SemaphoreType.DMA((2, chunks)),
        ],
        compiler_params=pltpu.CompilerParams(vmem_limit_bytes=12 << 20),
        cost_estimate=pl.CostEstimate(flops=4 * rows * total, bytes_accessed=10 * rows * total, transcendentals=0),
        name="mix",
    )(share, *arrays, *extra)


def join_kernel(a_ref, b_ref, out_ref):
    rows = a_ref.shape[0]
    out_ref[pl.ds(0, rows), :] = a_ref[...]
    out_ref[pl.ds(rows, b_ref.shape[0]), :] = b_ref[...]


def joined(a, b):
    shape = (a.shape[0] + b.shape[0], a.shape[1])
    a, b = (pltpu.with_memory_space_constraint(x, pltpu.VMEM) for x in (a, b))
    return pl.pallas_call(
        join_kernel,
        out_shape=pltpu.VMEM(shape, BF16),
        in_specs=[VMEM, VMEM],
        out_specs=VMEM,
        compiler_params=pltpu.CompilerParams(vmem_limit_bytes=4 << 20),
        cost_estimate=pl.CostEstimate(flops=shape[0] * shape[1], bytes_accessed=4 * shape[0] * shape[1], transcendentals=0),
        name="join",
    )(a, b)


def place_kernel(counts, by, join, *refs):
    extra = 1 if join else 0
    outs, sems = refs[-3 - extra : -1 - extra], refs[-1]
    joined = refs[-2] if join else None
    width = refs[0].shape[1]
    chips = lax.axis_size("zhi")
    chip, core = lax.axis_index("zhi"), lax.axis_index("core")
    sign = AHEAD * (1 - 2 * lax.axis_index("zlo"))
    copies, pieces, at = [], [], 0
    entries = iter(by)
    for ref, count in zip(refs, counts):
        row = 0
        for _ in range(count):
            which, start, size, step, other = next(entries)
            side = other - 2 if other > 1 else 1 - core if other else core
            owner = lax.rem(chip + chips - step * sign, chips) * 2 + side
            cols = pl.ds(pl.multiple_of(owner * width, width), width)
            piece = ref.at[pl.ds(row, size), :]
            row += size
            pieces.append((piece, size))
            copies.append(pltpu.make_async_copy(piece, outs[which].at[pl.ds(start, size), cols], sems.at[len(copies)]))
    for c in copies:
        c.start()
    if join:
        for piece, size in pieces[:join]:
            joined[pl.ds(at, size), :] = piece[...]
            at += size
    for c in copies:
        c.wait()


def placed(outs, arrays, columns, rows, join=0):
    n = len(arrays)
    by = tuple(p for _, pieces in arrays for p in pieces)
    counts = tuple(len(pieces) for _, pieces in arrays)
    arrays = [pltpu.with_memory_space_constraint(a, pltpu.VMEM) for a, _ in arrays]
    width = arrays[0].shape[1]
    total = sum(p[2] for p in by)
    joined = sum(p[2] for p in by[:join])
    out = jax.ShapeDtypeStruct((rows, columns), BF16)
    extra = () if outs is None else tuple(outs)
    res = pl.pallas_call(
        functools.partial(place_kernel, counts, by, join),
        out_shape=(out, out) + ((pltpu.VMEM((joined, width), BF16),) if join else ()),
        in_specs=[VMEM] * n + [ANY] * len(extra),
        out_specs=(ANY, ANY) + ((VMEM,) if join else ()),
        input_output_aliases={n + i: i for i in range(len(extra))},
        scratch_shapes=[pltpu.SemaphoreType.DMA((len(by),))],
        compiler_params=pltpu.CompilerParams(vmem_limit_bytes=12 << 20),
        cost_estimate=pl.CostEstimate(flops=2 * total * width, bytes_accessed=4 * total * width, transcendentals=0),
        name="place",
    )(*arrays, *extra)
    return res[:2], (res[2] if join else None)


def order_kernel(nxy, nz, in_ref, out_ref, wide):
    lanes = in_ref.shape[1]
    wide[...] = in_ref[...].astype(jnp.float32)
    column = in_ref.shape[0] // nxy
    for z in range(nz):
        for j in range(column // nz):
            rows = wide[pl.ds(z * (column // nz) + j, nxy, stride=column), :]
            out_ref[pl.ds(z * nxy, nxy), pl.ds(j * lanes, lanes)] = rows.astype(BF16)


def ordered(part, nxy, nz):
    rows, lanes = part.shape
    experts = nxy * nz
    return pl.pallas_call(
        functools.partial(order_kernel, nxy, nz),
        out_shape=jax.ShapeDtypeStruct((experts, rows * lanes // experts), BF16),
        in_specs=[VMEM],
        out_specs=VMEM,
        scratch_shapes=[
            pltpu.VMEM((rows, lanes), jnp.float32),
        ],
        compiler_params=pltpu.CompilerParams(vmem_limit_bytes=4 << 20),
        cost_estimate=pl.CostEstimate(flops=rows * lanes, bytes_accessed=4 * rows * lanes, transcendentals=0),
        name="order",
    )(part)


def spread(x, axes):
    n = lax.axis_size(axes)
    return lax.all_to_all(jnp.broadcast_to(x[None], (n, *x.shape)), axes, 0, 0, tiled=True)


def local(w_gate, avg_gate, w_up, avg_up, mix_share, router_weight, router_gain):
    chips = lax.axis_size("zhi")
    columns = w_gate.shape[1] * chips * lax.axis_size("core")
    rows = w_gate.shape[2]

    def moved(x, by):
        pairs = [
            (lo * chips + hi, lo * chips + (hi + (by if lo == 0 else -by)) % chips) for lo in range(2) for hi in range(chips)
        ]
        return lax.ppermute(x, ("zlo", "zhi"), pairs)

    def partner(x):
        return lax.ppermute(x, "core", [(0, 1), (1, 0)])

    def place(outs, *arrays, join=0):
        return placed(outs, arrays, columns, rows, join)

    def head(step, other):
        return ((GATE, 0, rows, step, other), (UP, 0, HEAD, step, other))

    def tail(step, other):
        return ((UP, HEAD, rows - HEAD, step, other),)

    (start,) = mixed(mix_share, ((w_gate[0], avg_gate[0], 0, FIRST),))
    more, first = mixed(
        mix_share,
        ((w_gate[0], avg_gate[0], FIRST, rows - FIRST), (w_up[0], avg_up[0], 0, HEAD)),
        start,
    )
    second, own = mixed(mix_share, ((w_up[0], avg_up[0], HEAD, rows - HEAD),), first)
    a0 = moved(start, AHEAD)
    a1 = moved(more, AHEAD)
    a2 = moved(second, AHEAD)
    a1 = joined(a0, a1)
    c1 = moved(a1, AHEAD)
    c2 = moved(a2, AHEAD)
    f1 = moved(c1, AHEAD)
    f2 = moved(c2, AHEAD)

    nx, ny, nz = (lax.axis_size(a) for a in ("x", "y", "zlo"))
    part = (router_weight * router_gain[:, None]).astype(BF16).reshape(2, -1)
    lanes = part.shape[1]
    part = spread(part, ("zlo", "zhi", "core")).reshape(-1, lanes)
    part = spread(part, ("y", "x")).reshape(-1, lanes)
    serve_router = ordered(part, nx * ny, nz).T

    outs, _ = place(None, (own, head(0, 0) + tail(0, 0)))
    outs, both = place(outs, (a1, head(1, 0)), (a2, tail(1, 0)), (partner(own), head(0, 1) + tail(0, 1)), join=3)
    outs, _ = place(outs, (partner(both), head(1, 1) + tail(1, 1)))
    outs, both = place(outs, (c1, head(2, 0)), (c2, tail(2, 0)), join=3)
    outs, _ = place(outs, (partner(both), head(2, 1) + tail(2, 1)), (f1, head(3, 0)), (partner(f1), head(3, 1)))
    last = lax.all_gather(f2, "core", axis=0, tiled=True)
    outs, _ = place(outs, (last, tail(3, 2) + tail(3, 3)))
    return outs[0][None], outs[1][None], serve_router


def solution(mesh):
    devices = mesh.devices.reshape(2, 8, 4, 4, 2)
    split = Mesh(devices, EXPERT + SHARD)
    return jax.shard_map(
        local,
        mesh=split,
        in_specs=(
            P(EXPERT, SHARD, None),
            P(EXPERT, SHARD, None),
            P(EXPERT, SHARD, None),
            P(EXPERT, SHARD, None),
            P(EXPERT),
            P(SHARD, EXPERT),
            P(SHARD),
        ),
        out_specs=(P(EXPERT, None, None), P(EXPERT, None, None), P()),
        check_vma=False,
    )
```

```python
import functools

import jax
import jax.numpy as jnp
from jax import lax
from jax.experimental import pallas as pl
from jax.experimental.pallas import tpu as pltpu
from jax.sharding import Mesh
from jax.sharding import PartitionSpec as P


BF16 = jnp.bfloat16
WIDTH = 256
HEAD = 256
FIRST = 512
EXPERT = ("zlo", "y", "x")
SHARD = ("zhi", "core")
ANY = pl.BlockSpec(memory_space=pl.ANY)
HBM = pl.BlockSpec(memory_space=pltpu.HBM)
VMEM = pl.BlockSpec(memory_space=pltpu.VMEM)
SMEM = pl.BlockSpec(memory_space=pltpu.SMEM)
GATE, UP = 0, 1
AHEAD = 1


def mix_kernel(plan, share_ref, *refs):
    n = len(plan)
    sources, before, outs, (buf, sems) = refs[: 2 * n], refs[2 * n : -4], refs[-4:-2], refs[-2:]
    width = buf.shape[-1]
    chunks, row = [], 0
    for i, (first, size) in enumerate(plan):
        for col in range(first, first + size, width):
            chunks.append((sources[2 * i], sources[2 * i + 1], col, min(width, first + size - col), row))
            row += chunks[-1][3]

    def copies(k):
        w, avg, col, size, _ = chunks[k]
        return [
            pltpu.make_async_copy(src.at[:, pl.ds(col, size)], buf.at[i, k, :, pl.ds(0, size)], sems.at[i, k])
            for i, src in enumerate((w, avg))
        ]

    for k in range(len(chunks)):
        for c in copies(k):
            c.start()
    share = share_ref[0]
    rest = 1.0 - share
    for k, (_, _, _, size, at) in enumerate(chunks):
        for c in copies(k):
            c.wait()
        fresh = share * buf[0, k, :, :size] + rest * buf[1, k, :, :size]
        turned = fresh.astype(BF16).T
        outs[0][pl.ds(at, size), :] = turned
        if before:
            outs[1][pl.ds(before[0].shape[0] + at, size), :] = turned
    if before:
        outs[1][pl.ds(0, before[0].shape[0]), :] = before[0][...]


def first_kernel(plan, *refs):
    mix_kernel(plan, *refs[:-2], None, *refs[-2:])


def mixed(share, sources, before=None):
    rows = sources[0][0].shape[0]
    plan = tuple((first, size) for _, _, first, size in sources)
    total = sum(size for _, size in plan)
    arrays = [pltpu.with_memory_space_constraint(x, pltpu.HBM) for w, avg, _, _ in sources for x in (w, avg)]
    extra = () if before is None else (pltpu.with_memory_space_constraint(before, pltpu.VMEM),)
    chunks = sum(-(-size // WIDTH) for _, size in plan)
    return pl.pallas_call(
        functools.partial(mix_kernel if extra else first_kernel, plan),
        out_shape=(pltpu.VMEM((total, rows), BF16),)
        + ((pltpu.VMEM((before.shape[0] + total, rows), BF16),) if extra else ()),
        in_specs=[SMEM] + [HBM] * len(arrays) + [VMEM] * len(extra),
        out_specs=(VMEM,) * (1 + len(extra)),
        scratch_shapes=[
            pltpu.VMEM((2, chunks, rows, WIDTH), jnp.float32),
            pltpu.SemaphoreType.DMA((2, chunks)),
        ],
        compiler_params=pltpu.CompilerParams(vmem_limit_bytes=12 << 20),
        cost_estimate=pl.CostEstimate(flops=4 * rows * total, bytes_accessed=10 * rows * total, transcendentals=0),
        name="mix",
    )(share, *arrays, *extra)


def join_kernel(a_ref, b_ref, out_ref):
    rows = a_ref.shape[0]
    out_ref[pl.ds(0, rows), :] = a_ref[...]
    out_ref[pl.ds(rows, b_ref.shape[0]), :] = b_ref[...]


def joined(a, b):
    shape = (a.shape[0] + b.shape[0], a.shape[1])
    a, b = (pltpu.with_memory_space_constraint(x, pltpu.VMEM) for x in (a, b))
    return pl.pallas_call(
        join_kernel,
        out_shape=pltpu.VMEM(shape, BF16),
        in_specs=[VMEM, VMEM],
        out_specs=VMEM,
        compiler_params=pltpu.CompilerParams(vmem_limit_bytes=4 << 20),
        cost_estimate=pl.CostEstimate(flops=shape[0] * shape[1], bytes_accessed=4 * shape[0] * shape[1], transcendentals=0),
        name="join",
    )(a, b)


def place_kernel(counts, by, join, *refs):
    extra = 1 if join else 0
    outs, sems = refs[-3 - extra : -1 - extra], refs[-1]
    joined = refs[-2] if join else None
    width = refs[0].shape[1]
    chips = lax.axis_size("zhi")
    chip, core = lax.axis_index("zhi"), lax.axis_index("core")
    sign = AHEAD * (1 - 2 * lax.axis_index("zlo"))
    copies, pieces, at = [], [], 0
    entries = iter(by)
    for ref, count in zip(refs, counts):
        row = 0
        for _ in range(count):
            which, start, size, step, other = next(entries)
            side = other - 2 if other > 1 else 1 - core if other else core
            owner = lax.rem(chip + chips - step * sign, chips) * 2 + side
            cols = pl.ds(pl.multiple_of(owner * width, width), width)
            piece = ref.at[pl.ds(row, size), :]
            row += size
            pieces.append((piece, size))
            copies.append(pltpu.make_async_copy(piece, outs[which].at[pl.ds(start, size), cols], sems.at[len(copies)]))
    for c in copies:
        c.start()
    if join:
        for piece, size in pieces[:join]:
            joined[pl.ds(at, size), :] = piece[...]
            at += size
    for c in copies:
        c.wait()


def placed(outs, arrays, columns, rows, join=0):
    n = len(arrays)
    by = tuple(p for _, pieces in arrays for p in pieces)
    counts = tuple(len(pieces) for _, pieces in arrays)
    arrays = [pltpu.with_memory_space_constraint(a, pltpu.VMEM) for a, _ in arrays]
    width = arrays[0].shape[1]
    total = sum(p[2] for p in by)
    joined = sum(p[2] for p in by[:join])
    out = jax.ShapeDtypeStruct((rows, columns), BF16)
    extra = () if outs is None else tuple(outs)
    res = pl.pallas_call(
        functools.partial(place_kernel, counts, by, join),
        out_shape=(out, out) + ((pltpu.VMEM((joined, width), BF16),) if join else ()),
        in_specs=[VMEM] * n + [ANY] * len(extra),
        out_specs=(ANY, ANY) + ((VMEM,) if join else ()),
        input_output_aliases={n + i: i for i in range(len(extra))},
        scratch_shapes=[pltpu.SemaphoreType.DMA((len(by),))],
        compiler_params=pltpu.CompilerParams(vmem_limit_bytes=12 << 20),
        cost_estimate=pl.CostEstimate(flops=2 * total * width, bytes_accessed=4 * total * width, transcendentals=0),
        name="place",
    )(*arrays, *extra)
    return res[:2], (res[2] if join else None)


def order_kernel(nxy, nz, in_ref, out_ref, wide):
    lanes = in_ref.shape[1]
    wide[...] = in_ref[...].astype(jnp.float32)
    column = in_ref.shape[0] // nxy
    for z in range(nz):
        for j in range(column // nz):
            rows = wide[pl.ds(z * (column // nz) + j, nxy, stride=column), :]
            out_ref[pl.ds(z * nxy, nxy), pl.ds(j * lanes, lanes)] = rows.astype(BF16)


def ordered(part, nxy, nz):
    rows, lanes = part.shape
    experts = nxy * nz
    return pl.pallas_call(
        functools.partial(order_kernel, nxy, nz),
        out_shape=jax.ShapeDtypeStruct((experts, rows * lanes // experts), BF16),
        in_specs=[VMEM],
        out_specs=VMEM,
        scratch_shapes=[
            pltpu.VMEM((rows, lanes), jnp.float32),
        ],
        compiler_params=pltpu.CompilerParams(vmem_limit_bytes=4 << 20),
        cost_estimate=pl.CostEstimate(flops=rows * lanes, bytes_accessed=4 * rows * lanes, transcendentals=0),
        name="order",
    )(part)


def spread(x, axes):
    n = lax.axis_size(axes)
    return lax.all_to_all(jnp.broadcast_to(x[None], (n, *x.shape)), axes, 0, 0, tiled=True)


def local(w_gate, avg_gate, w_up, avg_up, mix_share, router_weight, router_gain):
    chips = lax.axis_size("zhi")
    columns = w_gate.shape[1] * chips * lax.axis_size("core")
    rows = w_gate.shape[2]

    def moved(x, by):
        pairs = [
            (lo * chips + hi, lo * chips + (hi + (by if lo == 0 else -by)) % chips) for lo in range(2) for hi in range(chips)
        ]
        return lax.ppermute(x, ("zlo", "zhi"), pairs)

    def partner(x):
        return lax.ppermute(x, "core", [(0, 1), (1, 0)])

    def place(outs, *arrays, join=0):
        return placed(outs, arrays, columns, rows, join)

    def head(step, other):
        return ((GATE, 0, rows, step, other), (UP, 0, HEAD, step, other))

    def tail(step, other):
        return ((UP, HEAD, rows - HEAD, step, other),)

    (start,) = mixed(mix_share, ((w_gate[0], avg_gate[0], 0, FIRST),))
    more, first = mixed(
        mix_share,
        ((w_gate[0], avg_gate[0], FIRST, rows - FIRST), (w_up[0], avg_up[0], 0, HEAD)),
        start,
    )
    second, own = mixed(mix_share, ((w_up[0], avg_up[0], HEAD, rows - HEAD),), first)
    a0 = moved(start, AHEAD)
    a1 = moved(more, AHEAD)
    a2 = moved(second, AHEAD)
    a1 = joined(a0, a1)
    c1 = moved(a1, AHEAD)
    c2 = moved(a2, AHEAD)
    f1 = moved(c1, AHEAD)
    f2 = moved(c2, AHEAD)

    nx, ny, nz = (lax.axis_size(a) for a in ("x", "y", "zlo"))
    part = (router_weight * router_gain[:, None]).astype(BF16).reshape(2, -1)
    lanes = part.shape[1]
    part = spread(part, ("zlo", "zhi", "core")).reshape(-1, lanes)
    part = spread(part, ("y", "x")).reshape(-1, lanes)
    serve_router = ordered(part, nx * ny, nz).T

    outs, _ = place(None, (own, head(0, 0) + tail(0, 0)))
    d0 = partner(own)
    both = joined(a1, a2)
    d1 = partner(both)
    outs, _ = place(
        outs, (a1, head(1, 0)), (a2, tail(1, 0)), (d0, head(0, 1) + tail(0, 1)), (d1, head(1, 1) + tail(1, 1))
    )
    both = joined(c1, c2)
    d2 = partner(both)
    outs, _ = place(
        outs,
        (c1, head(2, 0)),
        (c2, tail(2, 0)),
        (d2, head(2, 1) + tail(2, 1)),
        (f1, head(3, 0)),
        (partner(f1), head(3, 1)),
    )
    last = lax.all_gather(f2, "core", axis=0, tiled=True)
    outs, _ = place(outs, (last, tail(3, 2) + tail(3, 3)))
    return outs[0][None], outs[1][None], serve_router


def solution(mesh):
    devices = mesh.devices.reshape(2, 8, 4, 4, 2)
    split = Mesh(devices, EXPERT + SHARD)
    return jax.shard_map(
        local,
        mesh=split,
        in_specs=(
            P(EXPERT, SHARD, None),
            P(EXPERT, SHARD, None),
            P(EXPERT, SHARD, None),
            P(EXPERT, SHARD, None),
            P(EXPERT),
            P(SHARD, EXPERT),
            P(SHARD),
        ),
        out_specs=(P(EXPERT, None, None), P(EXPERT, None, None), P()),
        check_vma=False,
    )
```

```python
import functools

import jax
import jax.numpy as jnp
from jax import lax
from jax.experimental import pallas as pl
from jax.experimental.pallas import tpu as pltpu
from jax.sharding import Mesh
from jax.sharding import PartitionSpec as P


BF16 = jnp.bfloat16
WIDTH = 256
HEAD = 256
EXPERT = ("zlo", "y", "x")
SHARD = ("zhi", "core")
ANY = pl.BlockSpec(memory_space=pl.ANY)
HBM = pl.BlockSpec(memory_space=pltpu.HBM)
VMEM = pl.BlockSpec(memory_space=pltpu.VMEM)
SMEM = pl.BlockSpec(memory_space=pltpu.SMEM)
GATE, UP = 0, 1
AHEAD = -1


def mix_kernel(first, size, share_ref, w, avg, before, out, whole, buf, sems):
    chunks = [(col, min(WIDTH, size - col)) for col in range(0, size, WIDTH)]

    def copies(k):
        col, wide = chunks[k]
        return [
            pltpu.make_async_copy(src.at[:, pl.ds(first + col, wide)], buf.at[i, k, :, pl.ds(0, wide)], sems.at[i, k])
            for i, src in enumerate((w, avg))
        ]

    for k in range(len(chunks)):
        for c in copies(k):
            c.start()
    share = share_ref[0]
    rest = 1.0 - share
    for k, (col, wide) in enumerate(chunks):
        for c in copies(k):
            c.wait()
        fresh = share * buf[0, k, :, :wide] + rest * buf[1, k, :, :wide]
        turned = fresh.astype(BF16).T
        out[pl.ds(col, wide), :] = turned
        whole[pl.ds(before.shape[0] + col, wide), :] = turned
    whole[pl.ds(0, before.shape[0]), :] = before[...]


def mark_kernel(out):
    out[...] = jnp.zeros(out.shape, out.dtype)


def marked():
    return pl.pallas_call(
        mark_kernel,
        out_shape=pltpu.VMEM((8, 128), jnp.float32),
        out_specs=VMEM,
        compiler_params=pltpu.CompilerParams(vmem_limit_bytes=1 << 20),
        cost_estimate=pl.CostEstimate(flops=1 << 34, bytes_accessed=1 << 24, transcendentals=0),
        name="mark",
    )()


def near_kernel(share_ref, w, avg, mark, out):
    share = share_ref[0]
    rest = 1.0 - share
    for col in range(0, w.shape[1], WIDTH):
        cols = pl.ds(col, WIDTH)
        fresh = share * w[:, cols] + rest * avg[:, cols]
        out[cols, :] = fresh.astype(BF16).T


def mixed_near(share, w, avg, mark):
    rows, columns = w.shape
    return pl.pallas_call(
        near_kernel,
        out_shape=pltpu.VMEM((columns, rows), BF16),
        in_specs=[SMEM] + [VMEM] * 3,
        out_specs=VMEM,
        compiler_params=pltpu.CompilerParams(vmem_limit_bytes=12 << 20),
        cost_estimate=pl.CostEstimate(flops=4 * rows * columns, bytes_accessed=10 * rows * columns, transcendentals=0),
        name="mix",
    )(share, *(pltpu.with_memory_space_constraint(x, pltpu.VMEM) for x in (w, avg, mark)))


def mixed(share, w, avg, first, size, before):
    rows = w.shape[0]
    w, avg = (pltpu.with_memory_space_constraint(x, pltpu.HBM) for x in (w, avg))
    chunks = -(-size // WIDTH)
    return pl.pallas_call(
        functools.partial(mix_kernel, first, size),
        out_shape=(pltpu.VMEM((size, rows), BF16), pltpu.VMEM((before.shape[0] + size, rows), BF16)),
        in_specs=[SMEM, HBM, HBM, VMEM],
        out_specs=(VMEM, VMEM),
        scratch_shapes=[
            pltpu.VMEM((2, chunks, rows, WIDTH), jnp.float32),
            pltpu.SemaphoreType.DMA((2, chunks)),
        ],
        compiler_params=pltpu.CompilerParams(vmem_limit_bytes=12 << 20),
        cost_estimate=pl.CostEstimate(flops=4 * rows * size, bytes_accessed=10 * rows * size, transcendentals=0),
        name="mix",
    )(share, w, avg, pltpu.with_memory_space_constraint(before, pltpu.VMEM))


def join_kernel(a_ref, b_ref, out_ref):
    rows = a_ref.shape[0]
    out_ref[pl.ds(0, rows), :] = a_ref[...]
    out_ref[pl.ds(rows, b_ref.shape[0]), :] = b_ref[...]


def joined(a, b):
    shape = (a.shape[0] + b.shape[0], a.shape[1])
    a, b = (pltpu.with_memory_space_constraint(x, pltpu.VMEM) for x in (a, b))
    return pl.pallas_call(
        join_kernel,
        out_shape=pltpu.VMEM(shape, BF16),
        in_specs=[VMEM, VMEM],
        out_specs=VMEM,
        compiler_params=pltpu.CompilerParams(vmem_limit_bytes=4 << 20),
        cost_estimate=pl.CostEstimate(flops=shape[0] * shape[1], bytes_accessed=4 * shape[0] * shape[1], transcendentals=0),
        name="join",
    )(a, b)


def place_kernel(counts, by, *refs):
    outs, sems = refs[-3:-1], refs[-1]
    width = refs[0].shape[1]
    chips = lax.axis_size("zhi")
    chip, core = lax.axis_index("zhi"), lax.axis_index("core")
    sign = AHEAD * (1 - 2 * lax.axis_index("zlo"))
    copies = []
    entries = iter(by)
    for ref, count in zip(refs, counts):
        row = 0
        for _ in range(count):
            which, start, size, step, other = next(entries)
            side = other - 2 if other > 1 else 1 - core if other else core
            owner = lax.rem(chip + chips - step * sign, chips) * 2 + side
            cols = pl.ds(pl.multiple_of(owner * width, width), width)
            piece = ref.at[pl.ds(row, size), :]
            row += size
            copies.append(pltpu.make_async_copy(piece, outs[which].at[pl.ds(start, size), cols], sems.at[len(copies)]))
    for c in copies:
        c.start()
    for c in copies:
        c.wait()


def placed(outs, arrays, columns, rows):
    n = len(arrays)
    by = tuple(p for _, pieces in arrays for p in pieces)
    counts = tuple(len(pieces) for _, pieces in arrays)
    arrays = [pltpu.with_memory_space_constraint(a, pltpu.VMEM) for a, _ in arrays]
    width = arrays[0].shape[1]
    total = sum(p[2] for p in by)
    out = jax.ShapeDtypeStruct((rows, columns), BF16)
    extra = () if outs is None else tuple(outs)
    return pl.pallas_call(
        functools.partial(place_kernel, counts, by),
        out_shape=(out, out),
        in_specs=[VMEM] * n + [ANY] * len(extra),
        out_specs=(ANY, ANY),
        input_output_aliases={n + i: i for i in range(len(extra))},
        scratch_shapes=[pltpu.SemaphoreType.DMA((len(by),))],
        compiler_params=pltpu.CompilerParams(vmem_limit_bytes=12 << 20),
        cost_estimate=pl.CostEstimate(flops=2 * total * width, bytes_accessed=4 * total * width, transcendentals=0),
        name="place",
    )(*arrays, *extra)


def order_kernel(nxy, nz, in_ref, out_ref, wide):
    lanes = in_ref.shape[1]
    wide[...] = in_ref[...].astype(jnp.float32)
    column = in_ref.shape[0] // nxy
    for z in range(nz):
        for j in range(column // nz):
            rows = wide[pl.ds(z * (column // nz) + j, nxy, stride=column), :]
            out_ref[pl.ds(z * nxy, nxy), pl.ds(j * lanes, lanes)] = rows.astype(BF16)


def ordered(part, nxy, nz):
    rows, lanes = part.shape
    experts = nxy * nz
    return pl.pallas_call(
        functools.partial(order_kernel, nxy, nz),
        out_shape=jax.ShapeDtypeStruct((experts, rows * lanes // experts), BF16),
        in_specs=[VMEM],
        out_specs=VMEM,
        scratch_shapes=[
            pltpu.VMEM((rows, lanes), jnp.float32),
        ],
        compiler_params=pltpu.CompilerParams(vmem_limit_bytes=4 << 20),
        cost_estimate=pl.CostEstimate(flops=rows * lanes, bytes_accessed=4 * rows * lanes, transcendentals=0),
        name="order",
    )(part)


def spread(x, axes):
    n = lax.axis_size(axes)
    return lax.all_to_all(jnp.broadcast_to(x[None], (n, *x.shape)), axes, 0, 0, tiled=True)


def local(w_gate, avg_gate, w_up, avg_up, mix_share, router_weight, router_gain):
    chips = lax.axis_size("zhi")
    columns = w_gate.shape[1] * chips * lax.axis_size("core")
    rows = w_gate.shape[2]

    def moved(x, by):
        pairs = [
            (lo * chips + hi, lo * chips + (hi + (by if lo == 0 else -by)) % chips) for lo in range(2) for hi in range(chips)
        ]
        return lax.ppermute(x, ("zlo", "zhi"), pairs)

    def partner(x):
        return lax.ppermute(x, "core", [(0, 1), (1, 0)])

    def place(outs, *arrays):
        return placed(outs, arrays, columns, rows)

    def head(step, other):
        return ((GATE, 0, rows, step, other), (UP, 0, HEAD, step, other))

    def tail(step, other):
        return ((UP, HEAD, rows - HEAD, step, other),)

    mark = marked()
    start = mixed_near(mix_share, w_gate[0], avg_gate[0], mark)
    more, first = mixed(mix_share, w_up[0], avg_up[0], 0, HEAD, start)
    second, own = mixed(mix_share, w_up[0], avg_up[0], HEAD, rows - HEAD, first)
    a0 = moved(start, AHEAD)
    a1 = moved(more, AHEAD)
    a2 = moved(second, AHEAD)
    a1 = joined(a0, a1)
    c1 = moved(a1, AHEAD)
    c2 = moved(a2, AHEAD)
    f1 = moved(c1, AHEAD)
    f2 = moved(c2, AHEAD)

    nx, ny, nz = (lax.axis_size(a) for a in ("x", "y", "zlo"))
    part = (router_weight * router_gain[:, None]).astype(BF16).reshape(2, -1)
    lanes = part.shape[1]
    part = spread(part, ("zlo", "zhi", "core")).reshape(-1, lanes)
    part = spread(part, ("y", "x")).reshape(-1, lanes)
    serve_router = ordered(part, nx * ny, nz).T

    outs = place(None, (own, head(0, 0) + tail(0, 0)))
    d0 = partner(own)
    both = joined(a1, a2)
    d1 = partner(both)
    outs = place(outs, (a1, head(1, 0)), (a2, tail(1, 0)), (d0, head(0, 1) + tail(0, 1)), (d1, head(1, 1) + tail(1, 1)))
    both = joined(c1, c2)
    d2 = partner(both)
    outs = place(
        outs,
        (c1, head(2, 0)),
        (c2, tail(2, 0)),
        (d2, head(2, 1) + tail(2, 1)),
        (f1, head(3, 0)),
        (partner(f1), head(3, 1)),
    )
    last = lax.all_gather(f2, "core", axis=0, tiled=True)
    outs = place(outs, (last, tail(3, 2) + tail(3, 3)))
    return outs[0][None], outs[1][None], serve_router


def solution(mesh):
    devices = mesh.devices.reshape(2, 8, 4, 4, 2)
    split = Mesh(devices, EXPERT + SHARD)
    return jax.shard_map(
        local,
        mesh=split,
        in_specs=(
            P(EXPERT, SHARD, None),
            P(EXPERT, SHARD, None),
            P(EXPERT, SHARD, None),
            P(EXPERT, SHARD, None),
            P(EXPERT),
            P(SHARD, EXPERT),
            P(SHARD),
        ),
        out_specs=(P(EXPERT, None, None), P(EXPERT, None, None), P()),
        check_vma=False,
    )
```

```python
import functools

import jax
import jax.numpy as jnp
from jax import lax
from jax.experimental import pallas as pl
from jax.experimental.pallas import tpu as pltpu
from jax.sharding import Mesh
from jax.sharding import PartitionSpec as P


BF16 = jnp.bfloat16
WIDTH = 256
HEAD = 256
EXPERT = ("zlo", "y", "x")
SHARD = ("zhi", "core")
ANY = pl.BlockSpec(memory_space=pl.ANY)
HBM = pl.BlockSpec(memory_space=pltpu.HBM)
VMEM = pl.BlockSpec(memory_space=pltpu.VMEM)
SMEM = pl.BlockSpec(memory_space=pltpu.SMEM)
GATE, UP = 0, 1
AHEAD = -1


def mix_kernel(first, size, share_ref, w, avg, before, out, whole, buf, sems):
    chunks = [(col, min(WIDTH, size - col)) for col in range(0, size, WIDTH)]

    def copies(k):
        col, wide = chunks[k]
        return [
            pltpu.make_async_copy(src.at[:, pl.ds(first + col, wide)], buf.at[i, k, :, pl.ds(0, wide)], sems.at[i, k])
            for i, src in enumerate((w, avg))
        ]

    for k in range(len(chunks)):
        for c in copies(k):
            c.start()
    share = share_ref[0]
    rest = 1.0 - share
    for k, (col, wide) in enumerate(chunks):
        for c in copies(k):
            c.wait()
        fresh = share * buf[0, k, :, :wide] + rest * buf[1, k, :, :wide]
        turned = fresh.astype(BF16).T
        out[pl.ds(col, wide), :] = turned
        whole[pl.ds(before.shape[0] + col, wide), :] = turned
    whole[pl.ds(0, before.shape[0]), :] = before[...]


def mark_kernel(out):
    out[...] = jnp.zeros(out.shape, out.dtype)


def marked():
    return pl.pallas_call(
        mark_kernel,
        out_shape=pltpu.VMEM((8, 128), jnp.float32),
        out_specs=VMEM,
        compiler_params=pltpu.CompilerParams(vmem_limit_bytes=1 << 20),
        cost_estimate=pl.CostEstimate(flops=1 << 34, bytes_accessed=1 << 24, transcendentals=0),
        name="mark",
    )()


def near_kernel(share_ref, w, avg, mark, out):
    share = share_ref[0]
    rest = 1.0 - share
    for col in range(0, w.shape[1], WIDTH):
        cols = pl.ds(col, WIDTH)
        fresh = share * w[:, cols] + rest * avg[:, cols]
        out[cols, :] = fresh.astype(BF16).T


def mixed_near(share, w, avg, mark):
    rows, columns = w.shape
    return pl.pallas_call(
        near_kernel,
        out_shape=pltpu.VMEM((columns, rows), BF16),
        in_specs=[SMEM] + [VMEM] * 3,
        out_specs=VMEM,
        compiler_params=pltpu.CompilerParams(vmem_limit_bytes=12 << 20),
        cost_estimate=pl.CostEstimate(flops=4 * rows * columns, bytes_accessed=10 * rows * columns, transcendentals=0),
        name="mix",
    )(share, *(pltpu.with_memory_space_constraint(x, pltpu.VMEM) for x in (w, avg, mark)))


def mixed(share, w, avg, first, size, before):
    rows = w.shape[0]
    w, avg = (pltpu.with_memory_space_constraint(x, pltpu.HBM) for x in (w, avg))
    chunks = -(-size // WIDTH)
    return pl.pallas_call(
        functools.partial(mix_kernel, first, size),
        out_shape=(pltpu.VMEM((size, rows), BF16), pltpu.VMEM((before.shape[0] + size, rows), BF16)),
        in_specs=[SMEM, HBM, HBM, VMEM],
        out_specs=(VMEM, VMEM),
        scratch_shapes=[
            pltpu.VMEM((2, chunks, rows, WIDTH), jnp.float32),
            pltpu.SemaphoreType.DMA((2, chunks)),
        ],
        compiler_params=pltpu.CompilerParams(vmem_limit_bytes=12 << 20),
        cost_estimate=pl.CostEstimate(flops=4 * rows * size, bytes_accessed=10 * rows * size, transcendentals=0),
        name="mix",
    )(share, w, avg, pltpu.with_memory_space_constraint(before, pltpu.VMEM))


def join_kernel(a_ref, b_ref, out_ref):
    rows = a_ref.shape[0]
    out_ref[pl.ds(0, rows), :] = a_ref[...]
    out_ref[pl.ds(rows, b_ref.shape[0]), :] = b_ref[...]


def joined(a, b):
    shape = (a.shape[0] + b.shape[0], a.shape[1])
    a, b = (pltpu.with_memory_space_constraint(x, pltpu.VMEM) for x in (a, b))
    return pl.pallas_call(
        join_kernel,
        out_shape=pltpu.VMEM(shape, BF16),
        in_specs=[VMEM, VMEM],
        out_specs=VMEM,
        compiler_params=pltpu.CompilerParams(vmem_limit_bytes=4 << 20),
        cost_estimate=pl.CostEstimate(flops=shape[0] * shape[1], bytes_accessed=4 * shape[0] * shape[1], transcendentals=0),
        name="join",
    )(a, b)


def place_kernel(counts, by, *refs):
    outs, sems = refs[-3:-1], refs[-1]
    width = refs[0].shape[1]
    chips = lax.axis_size("zhi")
    chip, core = lax.axis_index("zhi"), lax.axis_index("core")
    sign = AHEAD * (1 - 2 * lax.axis_index("zlo"))
    copies = []
    entries = iter(by)
    for ref, count in zip(refs, counts):
        row = 0
        for _ in range(count):
            which, start, size, step, other = next(entries)
            side = other - 2 if other > 1 else 1 - core if other else core
            owner = lax.rem(chip + chips - step * sign, chips) * 2 + side
            cols = pl.ds(pl.multiple_of(owner * width, width), width)
            piece = ref.at[pl.ds(row, size), :]
            row += size
            copies.append(pltpu.make_async_copy(piece, outs[which].at[pl.ds(start, size), cols], sems.at[len(copies)]))
    for c in copies:
        c.start()
    for c in copies:
        c.wait()


def placed(outs, arrays, columns, rows):
    n = len(arrays)
    by = tuple(p for _, pieces in arrays for p in pieces)
    counts = tuple(len(pieces) for _, pieces in arrays)
    arrays = [pltpu.with_memory_space_constraint(a, pltpu.VMEM) for a, _ in arrays]
    width = arrays[0].shape[1]
    total = sum(p[2] for p in by)
    out = jax.ShapeDtypeStruct((rows, columns), BF16)
    extra = () if outs is None else tuple(outs)
    return pl.pallas_call(
        functools.partial(place_kernel, counts, by),
        out_shape=(out, out),
        in_specs=[VMEM] * n + [ANY] * len(extra),
        out_specs=(ANY, ANY),
        input_output_aliases={n + i: i for i in range(len(extra))},
        scratch_shapes=[pltpu.SemaphoreType.DMA((len(by),))],
        compiler_params=pltpu.CompilerParams(vmem_limit_bytes=12 << 20),
        cost_estimate=pl.CostEstimate(flops=2 * total * width, bytes_accessed=4 * total * width, transcendentals=0),
        name="place",
    )(*arrays, *extra)


def order_kernel(nxy, nz, in_ref, out_ref, wide):
    lanes = in_ref.shape[1]
    wide[...] = in_ref[...].astype(jnp.float32)
    column = in_ref.shape[0] // nxy
    for z in range(nz):
        for j in range(column // nz):
            rows = wide[pl.ds(z * (column // nz) + j, nxy, stride=column), :]
            out_ref[pl.ds(z * nxy, nxy), pl.ds(j * lanes, lanes)] = rows.astype(BF16)


def ordered(part, nxy, nz):
    rows, lanes = part.shape
    experts = nxy * nz
    return pl.pallas_call(
        functools.partial(order_kernel, nxy, nz),
        out_shape=jax.ShapeDtypeStruct((experts, rows * lanes // experts), BF16),
        in_specs=[VMEM],
        out_specs=VMEM,
        scratch_shapes=[
            pltpu.VMEM((rows, lanes), jnp.float32),
        ],
        compiler_params=pltpu.CompilerParams(vmem_limit_bytes=4 << 20),
        cost_estimate=pl.CostEstimate(flops=rows * lanes, bytes_accessed=4 * rows * lanes, transcendentals=0),
        name="order",
    )(part)


def spread(x, axes):
    n = lax.axis_size(axes)
    return lax.all_to_all(jnp.broadcast_to(x[None], (n, *x.shape)), axes, 0, 0, tiled=True)


def local(w_gate, avg_gate, w_up, avg_up, mix_share, router_weight, router_gain):
    chips = lax.axis_size("zhi")
    columns = w_gate.shape[1] * chips * lax.axis_size("core")
    rows = w_gate.shape[2]

    def moved(x, by):
        pairs = [
            (lo * chips + hi, lo * chips + (hi + (by if lo == 0 else -by)) % chips) for lo in range(2) for hi in range(chips)
        ]
        return lax.ppermute(x, ("zlo", "zhi"), pairs)

    def partner(x):
        return lax.ppermute(x, "core", [(0, 1), (1, 0)])

    def place(outs, *arrays):
        return placed(outs, arrays, columns, rows)

    def head(step, other):
        return ((GATE, 0, rows, step, other), (UP, 0, HEAD, step, other))

    def tail(step, other):
        return ((UP, HEAD, rows - HEAD, step, other),)

    mark = marked()
    start = mixed_near(mix_share, w_gate[0], avg_gate[0], mark)
    more, first = mixed(mix_share, w_up[0], avg_up[0], 0, HEAD, start)
    second, own = mixed(mix_share, w_up[0], avg_up[0], HEAD, rows - HEAD, first)
    a0 = moved(start, AHEAD)
    a1 = moved(more, AHEAD)
    a2 = moved(second, AHEAD)
    a1 = joined(a0, a1)
    c1 = moved(a1, AHEAD)
    c2 = moved(a2, AHEAD)
    f1 = moved(c1, AHEAD)
    f2 = moved(c2, AHEAD)

    nx, ny, nz = (lax.axis_size(a) for a in ("x", "y", "zlo"))
    part = (router_weight * router_gain[:, None]).astype(BF16).reshape(2, -1)
    lanes = part.shape[1]
    part = spread(part, ("zlo", "zhi", "core")).reshape(-1, lanes)
    part = spread(part, ("y", "x")).reshape(-1, lanes)
    serve_router = ordered(part, nx * ny, nz).T

    d0 = partner(own)
    both = joined(a1, a2)
    d1 = partner(both)
    outs = place(
        None,
        (own, head(0, 0) + tail(0, 0)),
        (a1, head(1, 0)),
        (a2, tail(1, 0)),
        (d0, head(0, 1) + tail(0, 1)),
        (d1, head(1, 1) + tail(1, 1)),
    )
    both = joined(c1, c2)
    d2 = partner(both)
    outs = place(
        outs,
        (c1, head(2, 0)),
        (c2, tail(2, 0)),
        (d2, head(2, 1) + tail(2, 1)),
        (f1, head(3, 0)),
        (partner(f1), head(3, 1)),
    )
    last = lax.all_gather(f2, "core", axis=0, tiled=True)
    outs = place(outs, (last, tail(3, 2) + tail(3, 3)))
    return outs[0][None], outs[1][None], serve_router


def solution(mesh):
    devices = mesh.devices.reshape(2, 8, 4, 4, 2)
    split = Mesh(devices, EXPERT + SHARD)
    return jax.shard_map(
        local,
        mesh=split,
        in_specs=(
            P(EXPERT, SHARD, None),
            P(EXPERT, SHARD, None),
            P(EXPERT, SHARD, None),
            P(EXPERT, SHARD, None),
            P(EXPERT),
            P(SHARD, EXPERT),
            P(SHARD),
        ),
        out_specs=(P(EXPERT, None, None), P(EXPERT, None, None), P()),
        check_vma=False,
    )
```
